32 devices in a mesh: groups: 2 (over x), blk: 16 (over z, y, core).
Axes of the slice: x: 2, y: 2, z: 4, core: 2. Of those that a mesh axis runs over, the one named last changes fastest.
Arguments:
- coords: float32 [32, 24576], P(None, ('groups', 'blk')), parts along dimension 1, may hold values from -6 to 6
- alpha: float32 [24576], P(('groups', 'blk')), parts along dimension 0, may hold values from -6 to 6
- probe_solves: float32 [15, 24576], P(None, ('groups', 'blk')), parts along dimension 1, may hold values from -6 to 6
- probes: float32 [15, 24576], P(None, ('groups', 'blk')), parts along dimension 1, may hold values from -6 to 6
- lengthscale: float32 [32], replicated, may hold values from 4 to 12
Outputs:
- grad: float32 [32, 24576], P(None, ('groups', 'blk')), parts along dimension 1
The draws below stay inside these ranges and needn't reach their ends.
There are 2 independent parts, one for each index of `groups`. The reference program is written for one: setup_inputs(seed, part) draws one part's arguments, and reference() takes and returns one part's arrays. A program takes and returns all parts, laid end to end along the dimension named above; an argument that names none is the same for every part. Nothing has to cross between parts.
All inputs are finite; a program needn't handle non-finite values.
Results may differ from the reference program's by a relative error of at most 0.00014.
Values sent between devices are 32-bit elements; how exact they have to be, the bound alone decides.
A program may use at most 64 MiB of HBM per device.

```python
import math
import jax
import jax.numpy as jnp
from jax import lax

DIM = 32
PROBES = 15
BLOCK = 768
STEPS = 4
NPTS = 12288
N_BLK = 16


def levels(own_key, extent, shards, least, largest):
    level, own = 1.0, jax.random.fold_in(own_key, 6)
    for dim, blocks in shards:
        heights = jnp.exp(jax.random.uniform(jax.random.fold_in(own, dim), (blocks,), jnp.float32, least / len(shards), largest / len(shards)))
        level = level * jnp.repeat(heights, extent[dim] // blocks).reshape([-1 if axis == dim else 1 for axis in range(len(extent))])
    return level


def scatter_about(key, dims, deviation, most, split=(), dtype=jnp.bfloat16):
    drawn = deviation * jax.random.normal(key, dims, jnp.float32)
    if split:
        drawn = drawn * levels(key, dims, split, -0.22, 0.18)
    return jnp.clip(drawn, -most, most).astype(dtype)


def setup_inputs(seed: int = 0, part: int = 0) -> dict:
    seeds = jax.random.split(jax.random.key(seed), 6)
    part_splits = jax.random.split(jax.random.fold_in(seeds[5], part), 6)
    return {
        "coords": scatter_about(part_splits[0], (DIM, NPTS), 1.0, 6.0, ((1, 16),), jnp.float32),
        "alpha": scatter_about(part_splits[1], (NPTS,), 1.0, 6.0, ((0, 16),), jnp.float32),
        "probe_solves": scatter_about(part_splits[2], (PROBES, NPTS), 1.0, 6.0, ((1, 16),), jnp.float32),
        "probes": scatter_about(part_splits[3], (PROBES, NPTS), 1.0, 6.0, ((1, 16),), jnp.float32),
        "lengthscale": jnp.clip(jnp.exp(jax.random.uniform(seeds[4], (DIM,), jnp.float32, math.log(4.0), math.log(12.0))), 4.0, 12.0),
    }


root_five = 5.0 ** 0.5

def tile_terms(own_scaled, own_table, vis_scaled, vis_table):
    probe_count = (own_table.shape[0] - 1) // 2
    half_inv = 1.0 / (2.0 * probe_count)
    left_rows = jnp.concatenate([own_table[:1], -half_inv * own_table[1:]], 0)
    right_rows = jnp.concatenate([vis_table[:1], vis_table[1 + probe_count:], vis_table[1:1 + probe_count]], 0)
    contract_first = (((0,), (0,)), ((), ()))
    inner = lax.dot_general(own_scaled, vis_scaled, contract_first, precision=lax.Precision.HIGHEST, preferred_element_type=jnp.float32)
    own_square = lax.optimization_barrier(jnp.sum(own_scaled * own_scaled, 0))
    vis_square = lax.optimization_barrier(jnp.sum(vis_scaled * vis_scaled, 0))
    distance = own_square[:, None] + vis_square[None, :] - 2.0 * inner
    radius = jnp.sqrt(jnp.maximum(distance, 0.0))
    profile = (1.0 + root_five * radius) * jnp.exp(-root_five * radius)
    coupling = lax.dot_general(left_rows, right_rows, contract_first, precision=lax.Precision.HIGHEST, preferred_element_type=jnp.float32)
    weighted = coupling * profile
    row_part = own_scaled * lax.optimization_barrier(jnp.sum(weighted, 1))[None, :] - lax.dot_general(vis_scaled, weighted, (((1,), (1,)), ((), ())), precision=lax.Precision.HIGHEST, preferred_element_type=jnp.float32)
    col_part = vis_scaled * lax.optimization_barrier(jnp.sum(weighted, 0))[None, :] - jnp.dot(own_scaled, weighted, precision=lax.Precision.HIGHEST, preferred_element_type=jnp.float32)
    return (row_part, col_part)

def reference(coords, alpha, probe_solves, probes, lengthscale):
    scaled = coords / lengthscale[:, None]
    table = jnp.concatenate([alpha[None], probe_solves, probes], 0)
    blocks_scaled = scaled.reshape(DIM, N_BLK, BLOCK).transpose(1, 0, 2)
    blocks_table = table.reshape(table.shape[0], N_BLK, BLOCK).transpose(1, 0, 2)
    row_total = jnp.zeros(blocks_scaled.shape, jnp.float32)
    col_total = jnp.zeros(blocks_scaled.shape, jnp.float32)
    for offset in range(1, STEPS + 1):
        vis_scaled = jnp.roll(blocks_scaled, -offset, axis=0)
        vis_table = jnp.roll(blocks_table, -offset, axis=0)
        rows_now, cols_now = lax.map(lambda pieces: tile_terms(pieces[0], pieces[1], pieces[2], pieces[3]), (blocks_scaled, blocks_table, vis_scaled, vis_table))
        row_total = row_total + rows_now
        col_total = col_total + jnp.roll(cols_now, offset, axis=0)
    summed = (row_total + col_total).transpose(1, 0, 2).reshape(DIM, N_BLK * BLOCK)
    return -(5.0 / 3.0) / lengthscale[:, None] * summed
```

```python
import functools
import math

import jax
import jax.numpy as jnp
from jax import lax
from jax.experimental import pallas as pl
from jax.experimental.pallas import tpu as pltpu
from jax.sharding import PartitionSpec as P

unit = 5.0**0.5 * math.log2(math.e)
ln_two = math.log(2.0)
inv_ln_two = 1.0 / ln_two
f32, bf16 = jnp.float32, jnp.bfloat16
piece, chunk = 256, 256


def pieces(x):
    high = x.astype(bf16)
    rest = x - high.astype(f32)
    mid = rest.astype(bf16)
    low = (rest - mid.astype(f32)).astype(bf16)
    return high, mid, low


def norm_rows(field, own):
    high, mid, low = (p.astype(f32) for p in pieces(jnp.sum(field * field, 0, keepdims=True)))
    row = lax.broadcasted_iota(jnp.int32, (16, field.shape[1]), 0)
    first = 0 if own else 3
    ones = (row >= 3 - first) & (row < 6 - first)
    out = jnp.where(ones, 1.0, 0.0)
    for at, piece in enumerate((high, mid, low)):
        out = jnp.where(row == first + at, piece, out)
    return out.astype(bf16)


def kernel(
    dims, steps, count, coords, alpha, solves, probes, lengths, out,
    msg, line, held, held2, scales, recv, left_d, left_c, right_d, right_c, hold_d, hold_c, acc, load_sem, ready, send_sem, recv_sem,
):
    me = lax.axis_index("blk")
    core = lax.rem(me, 2)
    side = lax.rem(me // 2, 2)
    parts, rows, _ = msg.shape
    block = parts * piece
    width = (rows - dims) // 2

    def at(offset):
        return {"blk": lax.rem(me + offset + count, count)}

    partner = {"blk": me + 1 - 2 * core}
    mate = {"blk": me + 2 - 4 * side}
    reaches = range(4, steps + 1, 4)
    barrier = pltpu.get_barrier_semaphore()
    flip = 1 - 2 * side
    devices = [at(flip * k) for k in reaches] + [mate, partner]
    for device in devices:
        pl.semaphore_signal(barrier, inc=1, device_id=device, device_id_type=pl.DeviceIdType.MESH)

    loads = [(coords.at[:, pl.ds(p * piece, piece)], msg.at[p, pl.ds(0, dims), :]) for p in range(block // piece)]
    loads += [
        (solves, held),
        (probes, held2),
        (alpha, line),
        (lengths, scales),
    ]
    loads = [pltpu.make_async_copy(src, dst, load_sem.at[i]) for i, (src, dst) in enumerate(loads)]
    for load in loads:
        load.start()
    for load in loads:
        load.wait()
    extra = line[...].reshape(1, block)
    table = jnp.concatenate([held[...], extra, held2[...], jnp.zeros_like(extra)], 0)
    for p in range(parts):
        msg[p, dims:, :] = table[:, p * piece : (p + 1) * piece]
    pl.semaphore_wait(barrier, len(devices))

    copies = {}
    names = []

    def slot(name):
        if name not in names:
            names.append(name)
        return names.index(name)

    def send(src, name, part, device, now=True):
        copy = pltpu.make_async_remote_copy(
            src_ref=src.at[part],
            dst_ref=recv.at[slot(name), part],
            send_sem=send_sem.at[slot(name), part],
            recv_sem=recv_sem.at[slot(name), part],
            device_id=device,
            device_id_type=pl.DeviceIdType.MESH,
        )
        if now:
            copy.start()
        copies[name, part] = copy

    def arrive(name, part):
        copies[name, part].wait_recv()

    every = range(parts)

    def toward(name, k, part):
        send(msg, (name, k), part, at(-flip * k if name == "urgent" else flip * k))

    for i, k in enumerate(reaches):
        pl.semaphore_signal(ready.at[i], inc=1, device_id=at(-flip * k), device_id_type=pl.DeviceIdType.MESH)
    for part in every:
        for k in reaches:
            toward("urgent", k, part)
        send(msg, "mate", part, mate)
        send(msg, "partner", part, partner)
    dim = lax.broadcasted_iota(jnp.int32, (dims, 128), 0)
    length = jnp.full((dims, 128), 1.0, f32)
    for d in range(dims):
        length = jnp.where(dim == d, scales[d], length)
    length = length[:, :1]
    inverse = unit / length

    whole = jnp.concatenate([msg[p] for p in range(parts)], 1)
    field = whole[:dims, :] * inverse
    high, mid, low = pieces(-2.0 * field)
    left_d[...] = jnp.concatenate([high, high, high, norm_rows(field, True), mid, mid, low], 0).T
    row = lax.broadcasted_iota(jnp.int32, (width, block), 0)
    scale = math.e * ln_two / (2.0 * (width - 1))
    top, bottom = whole[dims : dims + width, :], whole[dims + width :, :]
    first = jnp.where(row == width - 1, -math.e * ln_two * top, scale * bottom)
    second = jnp.where(row == width - 1, 0.0, scale * top)
    high, mid, low = pieces(jnp.concatenate([first, second], 0))
    left_c[...] = jnp.concatenate([high, high, high, mid, mid, low], 0).T

    done = []
    pending = []
    contract = (((1,), (1,)), ((), ()))

    def finish(distance, coupling, buffer, lines, fresh):
        distance = jnp.maximum(distance, 1e-30)
        radius = distance * lax.rsqrt(distance)
        power = -inv_ln_two - radius
        weighted = coupling * power * jnp.exp2(power)
        w_high = weighted.astype(bf16)
        w_low = (weighted - w_high.astype(f32)).astype(bf16)
        across = right_d[buffer, : 3 * dims + 16, :]
        part_sum = lax.dot_general(across, w_high, contract, preferred_element_type=f32)
        part_sum += lax.dot_general(across, w_low, contract, preferred_element_type=f32)
        if fresh:
            acc[:, lines] = part_sum
        else:
            acc[:, lines] += part_sum

    def settle():
        if pending:
            finish(hold_d[...], hold_c[...], *pending.pop())

    def visit(*tiles):
        settle()
        for name, part in tiles:
            buffer, fresh = len(done) % 2, not done
            done.append(0)
            field = recv[slot(name), part, :dims, :] * inverse
            high, mid, low = pieces(field)
            right_d[buffer] = jnp.concatenate([high, mid, low, norm_rows(field, False), high, mid, high], 0)
            table = recv[slot(name), part, dims:, :]
            high, mid, low = pieces(table)
            right_c[buffer] = jnp.concatenate([high, mid, low, high, mid, high], 0)
            for start in range(0, block, chunk):
                lines = pl.ds(start, chunk)
                distance = jnp.dot(left_d[lines, :], right_d[buffer], preferred_element_type=f32)
                coupling = jnp.dot(left_c[lines, :], right_c[buffer], preferred_element_type=f32)
                if start + chunk == block and (name, part) == tiles[-1]:
                    hold_d[...] = distance
                    hold_c[...] = coupling
                    pending.append((buffer, lines, fresh))
                else:
                    finish(distance, coupling, buffer, lines, fresh)

    def land(name, part, onward=None, device=None, source=None):
        arrive(name, part)
        if onward is not None:
            send(recv.at[slot(name) if source is None else source], onward, part, device)

    for part in every:
        land("partner", part)
    visit(*[("partner", part) for part in every])
    for i, k in enumerate(reaches):
        pl.semaphore_wait(ready.at[i], 1)
        for part in every:
            toward("plain", k, part)

    last = steps
    inner = [(name, k) for k in reaches if k < last for name in ("urgent", "plain")]
    urgent, plain = ("urgent", last), ("plain", last)
    cross = jnp.where(core == side, slot(urgent), slot(plain))
    for part in every:
        land("mate", part, "mate2", partner)
        visit(("mate", part))
    for part in every:
        land(urgent, part, "over", mate)
        land("mate2", part)
        visit(("mate2", part), (urgent, part))
    for one in inner:
        for part in every:
            land(one, part, ("over", one), mate)
            send(recv.at[slot(one)], ("core", one), part, partner)
            visit((one, part))
    for part in every:
        land(plain, part, "cross", partner, cross)
        land("over", part, "over2", partner)
        visit((plain, part), ("over", part))
    for one in inner:
        for part in every:
            land(("over", one), part, ("over2", one), partner)
            land(("core", one), part)
            visit((("over", one), part), (("core", one), part))
            land(("over2", one), part)
            visit((("over2", one), part))
    for part in every:
        land("cross", part)
        land("over2", part)
        visit(("cross", part), ("over2", part))
    settle()
    total = acc[...]
    moved = total[:dims] + total[dims : 2 * dims] + total[2 * dims : 3 * dims]
    field = jnp.concatenate([msg[p, :dims, :] for p in range(parts)], 1) * inverse
    out[...] = (-(5.0 / 3.0) / unit / length) * (field * total[3 * dims : 3 * dims + 1] - moved)
    for copy in copies.values():
        copy.wait_send()


def on_device(coords, alpha, probe_solves, probes, lengthscale):
    count = lax.axis_size("blk")
    steps = count // 4
    dims, block = coords.shape
    table_rows = 2 * (probes.shape[0] + 1)
    rows = dims + table_rows
    depth_d, depth_c = 6 * dims + 16, 6 * table_rows
    parts = block // piece
    return pl.pallas_call(
        functools.partial(kernel, dims, steps, count),
        out_shape=pltpu.VMEM((dims, block), f32),
        in_specs=[pl.BlockSpec(memory_space=pltpu.HBM)] * 5,
        out_specs=pl.BlockSpec(memory_space=pltpu.VMEM),
        scratch_shapes=[
            pltpu.VMEM((parts, rows, piece), f32),
            pltpu.VMEM((block,), f32),
            pltpu.VMEM(probes.shape, f32),
            pltpu.VMEM(probes.shape, f32),
            pltpu.SMEM((dims,), f32),
            pltpu.VMEM((2 * steps, parts, rows, piece), f32),
            pltpu.VMEM((block, depth_d), bf16),
            pltpu.VMEM((block, depth_c), bf16),
            pltpu.VMEM((2, depth_d, piece), bf16),
            pltpu.VMEM((2, depth_c, piece), bf16),
            pltpu.VMEM((chunk, piece), f32),
            pltpu.VMEM((chunk, piece), f32),
            pltpu.VMEM((3 * dims + 16, block), f32),
            pltpu.SemaphoreType.DMA((parts + 4,)),
            pltpu.SemaphoreType.REGULAR((steps // 4,)),
            pltpu.SemaphoreType.DMA((2 * steps, parts)),
            pltpu.SemaphoreType.DMA((2 * steps, parts)),
        ],
        compiler_params=pltpu.CompilerParams(collective_id=0, has_side_effects=True),
    )(coords, alpha, probe_solves, probes, lengthscale)


def solution(mesh):
    return jax.shard_map(
        on_device,
        mesh=mesh,
        in_specs=(
            P(None, ("groups", "blk")),
            P(("groups", "blk")),
            P(None, ("groups", "blk")),
            P(None, ("groups", "blk")),
            P(),
        ),
        out_specs=P(None, ("groups", "blk")),
        check_vma=False,
    )
```

```python
import functools
import math

import jax
import jax.numpy as jnp
from jax import lax
from jax.experimental import pallas as pl
from jax.experimental.pallas import tpu as pltpu
from jax.sharding import PartitionSpec as P

unit = 5.0**0.5 * math.log2(math.e)
ln_two = math.log(2.0)
inv_ln_two = 1.0 / ln_two
f32, bf16 = jnp.float32, jnp.bfloat16
piece, chunk = 256, 128


def pieces(x):
    high = x.astype(bf16)
    rest = x - high.astype(f32)
    mid = rest.astype(bf16)
    low = (rest - mid.astype(f32)).astype(bf16)
    return high, mid, low


def norm_rows(field, own):
    high, mid, low = (p.astype(f32) for p in pieces(jnp.sum(field * field, 0, keepdims=True)))
    row = lax.broadcasted_iota(jnp.int32, (16, field.shape[1]), 0)
    first = 0 if own else 3
    ones = (row >= 3 - first) & (row < 6 - first)
    out = jnp.where(ones, 1.0, 0.0)
    for at, piece in enumerate((high, mid, low)):
        out = jnp.where(row == first + at, piece, out)
    return out.astype(bf16)


def kernel(
    dims, steps, count, coords, alpha, solves, probes, lengths, out,
    msg, line, held, held2, scales, recv, left_d, left_c, right_d, right_c, hold_d, hold_c, acc, load_sem, send_sem, recv_sem,
):
    me = lax.axis_index("blk")
    core = lax.rem(me, 2)
    side = lax.rem(me // 2, 2)
    parts, rows, _ = msg.shape
    block = parts * piece
    width = (rows - dims) // 2

    def at(offset):
        return {"blk": lax.rem(me + offset + count, count)}

    partner = {"blk": me + 1 - 2 * core}
    mate = {"blk": me + 2 - 4 * side}
    reaches = range(4, steps + 1, 4)
    barrier = pltpu.get_barrier_semaphore()
    flip = 1 - 2 * side
    devices = [at(sign * k) for k in reaches for sign in (1, -1)] + [mate, partner]
    for device in devices:
        pl.semaphore_signal(barrier, inc=1, device_id=device, device_id_type=pl.DeviceIdType.MESH)

    loads = [(coords.at[:, pl.ds(p * piece, piece)], msg.at[p, pl.ds(0, dims), :]) for p in range(block // piece)]
    loads += [
        (solves, held),
        (probes, held2),
        (alpha, line),
        (lengths, scales),
    ]
    loads = [pltpu.make_async_copy(src, dst, load_sem.at[i]) for i, (src, dst) in enumerate(loads)]
    for load in loads:
        load.start()
    for load in loads:
        load.wait()
    extra = line[...].reshape(1, block)
    table = jnp.concatenate([held[...], extra, held2[...], jnp.zeros_like(extra)], 0)
    for p in range(parts):
        msg[p, dims:, :] = table[:, p * piece : (p + 1) * piece]
    pl.semaphore_wait(barrier, len(devices))

    copies = {}
    names = []

    def slot(name):
        if name not in names:
            names.append(name)
        return names.index(name)

    def send(src, name, part, device, now=True):
        copy = pltpu.make_async_remote_copy(
            src_ref=src.at[part],
            dst_ref=recv.at[slot(name), part],
            send_sem=send_sem.at[slot(name), part],
            recv_sem=recv_sem.at[slot(name), part],
            device_id=device,
            device_id_type=pl.DeviceIdType.MESH,
        )
        if now:
            copy.start()
        copies[name, part] = copy

    def arrive(name, part):
        copies[name, part].wait_recv()

    every = range(parts)

    def toward(name, k, part):
        send(msg, (name, k), part, at(-flip * k if name == "urgent" else flip * k))

    for part in every:
        for k in reaches:
            send(msg, ("urgent", k), part, at(-flip * k), False)
            send(msg, ("plain", k), part, at(flip * k), False)

    def start(order):
        for name, part in order:
            for k in reaches:
                copies[(name, k), part].start()

    start([("urgent", part) for part in every])
    for part in every:
        send(msg, "mate", part, mate)
    for part in every:
        send(msg, "partner", part, partner)
    start([("plain", part) for part in every])

    dim = lax.broadcasted_iota(jnp.int32, (dims, 128), 0)
    length = jnp.full((dims, 128), 1.0, f32)
    for d in range(dims):
        length = jnp.where(dim == d, scales[d], length)
    length = length[:, :1]
    inverse = unit / length

    whole = jnp.concatenate([msg[p] for p in range(parts)], 1)
    field = whole[:dims, :] * inverse
    high, mid, low = pieces(-2.0 * field)
    left_d[...] = jnp.concatenate([high, high, high, norm_rows(field, True), mid, mid, low], 0).T
    row = lax.broadcasted_iota(jnp.int32, (width, block), 0)
    scale = math.e * ln_two / (2.0 * (width - 1))
    top, bottom = whole[dims : dims + width, :], whole[dims + width :, :]
    first = jnp.where(row == width - 1, -math.e * ln_two * top, scale * bottom)
    second = jnp.where(row == width - 1, 0.0, scale * top)
    high, mid, low = pieces(jnp.concatenate([first, second], 0))
    left_c[...] = jnp.concatenate([high, high, high, mid, mid, low], 0).T

    done = []
    pending = []
    contract = (((1,), (1,)), ((), ()))

    def finish(distance, coupling, buffer, lines, fresh):
        distance = jnp.maximum(distance, 1e-30)
        radius = distance * lax.rsqrt(distance)
        power = -inv_ln_two - radius
        weighted = coupling * power * jnp.exp2(power)
        w_high = weighted.astype(bf16)
        w_low = (weighted - w_high.astype(f32)).astype(bf16)
        across = right_d[buffer, : 3 * dims + 16, :]
        part_sum = lax.dot_general(across, w_high, contract, preferred_element_type=f32)
        part_sum += lax.dot_general(across, w_low, contract, preferred_element_type=f32)
        if fresh:
            acc[:, lines] = part_sum
        else:
            acc[:, lines] += part_sum

    def settle():
        if pending:
            finish(hold_d[...], hold_c[...], *pending.pop())

    def visit(*tiles):
        settle()
        for name, part in tiles:
            buffer, fresh = len(done) % 2, not done
            done.append(0)
            field = recv[slot(name), part, :dims, :] * inverse
            high, mid, low = pieces(field)
            right_d[buffer] = jnp.concatenate([high, mid, low, norm_rows(field, False), high, mid, high], 0)
            table = recv[slot(name), part, dims:, :]
            high, mid, low = pieces(table)
            right_c[buffer] = jnp.concatenate([high, mid, low, high, mid, high], 0)
            for start in range(0, block, chunk):
                lines = pl.ds(start, chunk)
                distance = jnp.dot(left_d[lines, :], right_d[buffer], preferred_element_type=f32)
                coupling = jnp.dot(left_c[lines, :], right_c[buffer], preferred_element_type=f32)
                if start + chunk == block and (name, part) == tiles[-1]:
                    hold_d[...] = distance
                    hold_c[...] = coupling
                    pending.append((buffer, lines, fresh))
                else:
                    finish(distance, coupling, buffer, lines, fresh)

    def land(name, part, onward=None, device=None, source=None):
        arrive(name, part)
        if onward is not None:
            send(recv.at[slot(name) if source is None else source], onward, part, device)

    for part in every:
        land("partner", part)
    visit(*[("partner", part) for part in every])
    last = steps
    inner = [(name, k) for k in reaches if k < last for name in ("urgent", "plain")]
    urgent, plain = ("urgent", last), ("plain", last)
    cross = jnp.where(core == side, slot(urgent), slot(plain))
    for part in every:
        land("mate", part, "mate2", partner)
        land(urgent, part, "over", mate)
        if part:
            land("mate2", part - 1)
            visit(("mate2", part - 1), ("mate", part), (urgent, part))
        else:
            visit(("mate", part), (urgent, part))
    land("mate2", parts - 1)
    visit(("mate2", parts - 1))
    for one in inner:
        for part in every:
            land(one, part, ("over", one), mate)
            send(recv.at[slot(one)], ("core", one), part, partner)
            visit((one, part))
    for part in every:
        land(plain, part, "cross", partner, cross)
        land("over", part, "over2", partner)
        if part:
            land("cross", part - 1)
            land("over2", part - 1)
            visit((plain, part), ("over", part), ("cross", part - 1), ("over2", part - 1))
        else:
            visit((plain, part), ("over", part))
    land("cross", parts - 1)
    land("over2", parts - 1)
    visit(("cross", parts - 1), ("over2", parts - 1))
    for one in inner:
        for part in every:
            land(("over", one), part, ("over2", one), partner)
            land(("core", one), part)
            visit((("over", one), part), (("core", one), part))
            land(("over2", one), part)
            visit((("over2", one), part))
    settle()
    total = acc[...]
    moved = total[:dims] + total[dims : 2 * dims] + total[2 * dims : 3 * dims]
    field = jnp.concatenate([msg[p, :dims, :] for p in range(parts)], 1) * inverse
    out[...] = (-(5.0 / 3.0) / unit / length) * (field * total[3 * dims : 3 * dims + 1] - moved)
    for copy in copies.values():
        copy.wait_send()


def on_device(coords, alpha, probe_solves, probes, lengthscale):
    count = lax.axis_size("blk")
    steps = count // 4
    dims, block = coords.shape
    table_rows = 2 * (probes.shape[0] + 1)
    rows = dims + table_rows
    depth_d, depth_c = 6 * dims + 16, 6 * table_rows
    parts = block // piece
    return pl.pallas_call(
        functools.partial(kernel, dims, steps, count),
        out_shape=pltpu.VMEM((dims, block), f32),
        in_specs=[pl.BlockSpec(memory_space=pltpu.HBM)] * 5,
        out_specs=pl.BlockSpec(memory_space=pltpu.VMEM),
        scratch_shapes=[
            pltpu.VMEM((parts, rows, piece), f32),
            pltpu.VMEM((block,), f32),
            pltpu.VMEM(probes.shape, f32),
            pltpu.VMEM(probes.shape, f32),
            pltpu.SMEM((dims,), f32),
            pltpu.VMEM((2 * steps, parts, rows, piece), f32),
            pltpu.VMEM((block, depth_d), bf16),
            pltpu.VMEM((block, depth_c), bf16),
            pltpu.VMEM((2, depth_d, piece), bf16),
            pltpu.VMEM((2, depth_c, piece), bf16),
            pltpu.VMEM((chunk, piece), f32),
            pltpu.VMEM((chunk, piece), f32),
            pltpu.VMEM((3 * dims + 16, block), f32),
            pltpu.SemaphoreType.DMA((parts + 4,)),
            pltpu.SemaphoreType.DMA((2 * steps, parts)),
            pltpu.SemaphoreType.DMA((2 * steps, parts)),
        ],
        compiler_params=pltpu.CompilerParams(collective_id=0, has_side_effects=True),
    )(coords, alpha, probe_solves, probes, lengthscale)


def solution(mesh):
    return jax.shard_map(
        on_device,
        mesh=mesh,
        in_specs=(
            P(None, ("groups", "blk")),
            P(("groups", "blk")),
            P(None, ("groups", "blk")),
            P(None, ("groups", "blk")),
            P(),
        ),
        out_specs=P(None, ("groups", "blk")),
        check_vma=False,
    )
```

```python
import functools
import math

import jax
import jax.numpy as jnp
from jax import lax
from jax.experimental import pallas as pl
from jax.experimental.pallas import tpu as pltpu
from jax.sharding import PartitionSpec as P

unit = 5.0**0.5 * math.log2(math.e)
ln_two = math.log(2.0)
inv_ln_two = 1.0 / ln_two
f32, bf16 = jnp.float32, jnp.bfloat16
piece, chunk = 256, 128


def pieces(x):
    high = x.astype(bf16)
    rest = x - high.astype(f32)
    mid = rest.astype(bf16)
    low = (rest - mid.astype(f32)).astype(bf16)
    return high, mid, low


def norm_rows(field, own):
    high, mid, low = (p.astype(f32) for p in pieces(jnp.sum(field * field, 0, keepdims=True)))
    row = lax.broadcasted_iota(jnp.int32, (16, field.shape[1]), 0)
    first = 0 if own else 3
    ones = (row >= 3 - first) & (row < 6 - first)
    out = jnp.where(ones, 1.0, 0.0)
    for at, piece in enumerate((high, mid, low)):
        out = jnp.where(row == first + at, piece, out)
    return out.astype(bf16)


def kernel(
    dims, steps, count, coords, alpha, solves, probes, lengths, out,
    msg, line, held, held2, scales, recv, left_d, left_c, right_d, right_c, hold_d, hold_c, acc, load_sem, ready, send_sem, recv_sem,
):
    me = lax.axis_index("blk")
    core = lax.rem(me, 2)
    side = lax.rem(me // 2, 2)
    parts, rows, _ = msg.shape
    block = parts * piece
    width = (rows - dims) // 2

    def at(offset):
        return {"blk": lax.rem(me + offset + count, count)}

    partner = {"blk": me + 1 - 2 * core}
    mate = {"blk": me + 2 - 4 * side}
    reaches = range(4, steps + 1, 4)
    barrier = pltpu.get_barrier_semaphore()
    flip = 1 - 2 * side
    devices = [at(flip * k) for k in reaches] + [mate, partner]
    for device in devices:
        pl.semaphore_signal(barrier, inc=1, device_id=device, device_id_type=pl.DeviceIdType.MESH)

    loads = [(coords.at[:, pl.ds(p * piece, piece)], msg.at[p, pl.ds(0, dims), :]) for p in range(block // piece)]
    loads += [
        (solves, held),
        (probes, held2),
        (alpha, line),
        (lengths, scales),
    ]
    loads = [pltpu.make_async_copy(src, dst, load_sem.at[i]) for i, (src, dst) in enumerate(loads)]
    for load in loads:
        load.start()
    for load in loads:
        load.wait()
    extra = line[...].reshape(1, block)
    table = jnp.concatenate([held[...], extra, held2[...], jnp.zeros_like(extra)], 0)
    for p in range(parts):
        msg[p, dims:, :] = table[:, p * piece : (p + 1) * piece]
    pl.semaphore_wait(barrier, len(devices))

    copies = {}
    names = []

    def slot(name):
        if name not in names:
            names.append(name)
        return names.index(name)

    def send(src, name, part, device):
        copy = pltpu.make_async_remote_copy(
            src_ref=src.at[part],
            dst_ref=recv.at[slot(name), part],
            send_sem=send_sem.at[slot(name), part],
            recv_sem=recv_sem.at[slot(name), part],
            device_id=device,
            device_id_type=pl.DeviceIdType.MESH,
        )
        copy.start()
        copies[name, part] = copy

    def arrive(name, part):
        copies[name, part].wait_recv()

    every = range(parts)

    for i, k in enumerate(reaches):
        pl.semaphore_signal(ready.at[i], inc=1, device_id=at(-flip * k), device_id_type=pl.DeviceIdType.MESH)
    for part in every:
        for k in reaches:
            send(msg, ("urgent", k), part, at(-flip * k))
        send(msg, "mate", part, mate)
    for part in every:
        send(msg, "partner", part, partner)

    dim = lax.broadcasted_iota(jnp.int32, (dims, 128), 0)
    length = jnp.full((dims, 128), 1.0, f32)
    for d in range(dims):
        length = jnp.where(dim == d, scales[d], length)
    length = length[:, :1]
    inverse = unit / length

    whole = jnp.concatenate([msg[p] for p in range(parts)], 1)
    field = whole[:dims, :] * inverse
    high, mid, low = pieces(-2.0 * field)
    left_d[...] = jnp.concatenate([high, high, high, norm_rows(field, True), mid, mid, low], 0).T
    row = lax.broadcasted_iota(jnp.int32, (width, block), 0)
    scale = math.e * ln_two / (2.0 * (width - 1))
    top, bottom = whole[dims : dims + width, :], whole[dims + width :, :]
    first = jnp.where(row == width - 1, -math.e * ln_two * top, scale * bottom)
    second = jnp.where(row == width - 1, 0.0, scale * top)
    high, mid, low = pieces(jnp.concatenate([first, second], 0))
    left_c[...] = jnp.concatenate([high, high, high, mid, mid, low], 0).T

    done = []
    pending = []
    contract = (((1,), (1,)), ((), ()))

    def finish(distance, coupling, buffer, lines, fresh):
        distance = jnp.maximum(distance, 1e-30)
        radius = distance * lax.rsqrt(distance)
        power = -inv_ln_two - radius
        weighted = coupling * power * jnp.exp2(power)
        w_high = weighted.astype(bf16)
        w_low = (weighted - w_high.astype(f32)).astype(bf16)
        across = right_d[buffer, : 3 * dims + 16, :]
        part_sum = lax.dot_general(across, w_high, contract, preferred_element_type=f32)
        part_sum += lax.dot_general(across, w_low, contract, preferred_element_type=f32)
        if fresh:
            acc[:, lines] = part_sum
        else:
            acc[:, lines] += part_sum

    def settle():
        if pending:
            finish(hold_d[...], hold_c[...], *pending.pop())

    def visit(*tiles):
        settle()
        for name, part in tiles:
            buffer, fresh = len(done) % 2, not done
            done.append(0)
            field = recv[slot(name), part, :dims, :] * inverse
            high, mid, low = pieces(field)
            right_d[buffer] = jnp.concatenate([high, mid, low, norm_rows(field, False), high, mid, high], 0)
            table = recv[slot(name), part, dims:, :]
            high, mid, low = pieces(table)
            right_c[buffer] = jnp.concatenate([high, mid, low, high, mid, high], 0)
            for start in range(0, block, chunk):
                lines = pl.ds(start, chunk)
                coupling = jnp.dot(left_c[lines, :], right_c[buffer], preferred_element_type=f32)
                distance = jnp.dot(left_d[lines, :], right_d[buffer], preferred_element_type=f32)
                if start + chunk == block and (name, part) == tiles[-1]:
                    hold_d[...] = distance
                    hold_c[...] = coupling
                    pending.append((buffer, lines, fresh))
                else:
                    finish(distance, coupling, buffer, lines, fresh)

    def land(name, part, onward=None, device=None, source=None):
        arrive(name, part)
        if onward is not None:
            send(recv.at[slot(name) if source is None else source], onward, part, device)

    for part in every:
        land("partner", part)
    visit(*[("partner", part) for part in every])
    for i, k in enumerate(reaches):
        pl.semaphore_wait(ready.at[i], 1)
        for part in every:
            send(msg, ("plain", k), part, at(flip * k))
    last = steps
    inner = [(name, k) for k in reaches if k < last for name in ("urgent", "plain")]
    urgent, plain = ("urgent", last), ("plain", last)
    cross = jnp.where(core == side, slot(urgent), slot(plain))
    for part in every:
        land("mate", part, "mate2", partner)
        land(urgent, part, "over", mate)
        if part:
            land("mate2", part - 1)
            visit(("mate2", part - 1), ("mate", part), (urgent, part))
        else:
            visit(("mate", part), (urgent, part))
    land("mate2", parts - 1)
    visit(("mate2", parts - 1))
    for one in inner:
        for part in every:
            land(one, part, ("over", one), mate)
            send(recv.at[slot(one)], ("core", one), part, partner)
            visit((one, part))
    for part in every:
        land("over", part, "over2", partner)
        land(plain, part, "cross", partner, cross)
        if part:
            land("cross", part - 1)
            land("over2", part - 1)
            visit((plain, part), ("over", part), ("cross", part - 1), ("over2", part - 1))
        else:
            visit((plain, part), ("over", part))
    land("cross", parts - 1)
    land("over2", parts - 1)
    visit(("cross", parts - 1), ("over2", parts - 1))
    for one in inner:
        for part in every:
            land(("over", one), part, ("over2", one), partner)
            land(("core", one), part)
            visit((("over", one), part), (("core", one), part))
            land(("over2", one), part)
            visit((("over2", one), part))
    settle()
    total = acc[...]
    moved = total[:dims] + total[dims : 2 * dims] + total[2 * dims : 3 * dims]
    field = jnp.concatenate([msg[p, :dims, :] for p in range(parts)], 1) * inverse
    out[...] = (-(5.0 / 3.0) / unit / length) * (field * total[3 * dims : 3 * dims + 1] - moved)
    for copy in copies.values():
        copy.wait_send()


def on_device(coords, alpha, probe_solves, probes, lengthscale):
    count = lax.axis_size("blk")
    steps = count // 4
    dims, block = coords.shape
    table_rows = 2 * (probes.shape[0] + 1)
    rows = dims + table_rows
    depth_d, depth_c = 6 * dims + 16, 6 * table_rows
    parts = block // piece
    return pl.pallas_call(
        functools.partial(kernel, dims, steps, count),
        out_shape=pltpu.VMEM((dims, block), f32),
        in_specs=[pl.BlockSpec(memory_space=pltpu.HBM)] * 5,
        out_specs=pl.BlockSpec(memory_space=pltpu.VMEM),
        scratch_shapes=[
            pltpu.VMEM((parts, rows, piece), f32),
            pltpu.VMEM((block,), f32),
            pltpu.VMEM(probes.shape, f32),
            pltpu.VMEM(probes.shape, f32),
            pltpu.SMEM((dims,), f32),
            pltpu.VMEM((2 * steps, parts, rows, piece), f32),
            pltpu.VMEM((block, depth_d), bf16),
            pltpu.VMEM((block, depth_c), bf16),
            pltpu.VMEM((2, depth_d, piece), bf16),
            pltpu.VMEM((2, depth_c, piece), bf16),
            pltpu.VMEM((chunk, piece), f32),
            pltpu.VMEM((chunk, piece), f32),
            pltpu.VMEM((3 * dims + 16, block), f32),
            pltpu.SemaphoreType.DMA((parts + 4,)),
            pltpu.SemaphoreType.REGULAR((steps // 4,)),
            pltpu.SemaphoreType.DMA((2 * steps, parts)),
            pltpu.SemaphoreType.DMA((2 * steps, parts)),
        ],
        compiler_params=pltpu.CompilerParams(collective_id=0, has_side_effects=True),
    )(coords, alpha, probe_solves, probes, lengthscale)


def solution(mesh):
    return jax.shard_map(
        on_device,
        mesh=mesh,
        in_specs=(
            P(None, ("groups", "blk")),
            P(("groups", "blk")),
            P(None, ("groups", "blk")),
            P(None, ("groups", "blk")),
            P(),
        ),
        out_specs=P(None, ("groups", "blk")),
        check_vma=False,
    )
```

```python
import functools
import math

import jax
import jax.numpy as jnp
from jax import lax
from jax.experimental import pallas as pl
from jax.experimental.pallas import tpu as pltpu
from jax.sharding import PartitionSpec as P

unit = 5.0**0.5 * math.log2(math.e)
ln_two = math.log(2.0)
inv_ln_two = 1.0 / ln_two
f32, bf16 = jnp.float32, jnp.bfloat16
piece, chunk, kept = 256, 128, 2


def pieces(x):
    high = x.astype(bf16)
    rest = x - high.astype(f32)
    mid = rest.astype(bf16)
    low = (rest - mid.astype(f32)).astype(bf16)
    return high, mid, low


def norm_rows(field, own):
    high, mid, low = (p.astype(f32) for p in pieces(jnp.sum(field * field, 0, keepdims=True)))
    row = lax.broadcasted_iota(jnp.int32, (16, field.shape[1]), 0)
    first = 0 if own else 3
    ones = (row >= 3 - first) & (row < 6 - first)
    out = jnp.where(ones, 1.0, 0.0)
    for at, piece in enumerate((high, mid, low)):
        out = jnp.where(row == first + at, piece, out)
    return out.astype(bf16)


def kernel(
    dims, steps, count, coords, alpha, solves, probes, lengths, out,
    msg, line, held, held2, scales, recv, left_d, left_c, right_d, right_c, hold_d, hold_c, acc, load_sem, ready, send_sem, recv_sem,
):
    me = lax.axis_index("blk")
    core = lax.rem(me, 2)
    side = lax.rem(me // 2, 2)
    parts, rows, _ = msg.shape
    block = parts * piece
    width = (rows - dims) // 2

    def at(offset):
        return {"blk": lax.rem(me + offset + count, count)}

    partner = {"blk": me + 1 - 2 * core}
    mate = {"blk": me + 2 - 4 * side}
    reaches = range(4, steps + 1, 4)
    barrier = pltpu.get_barrier_semaphore()
    flip = 1 - 2 * side
    devices = [at(flip * k) for k in reaches] + [mate, partner]
    for device in devices:
        pl.semaphore_signal(barrier, inc=1, device_id=device, device_id_type=pl.DeviceIdType.MESH)

    loads = [(coords.at[:, pl.ds(p * piece, piece)], msg.at[p, pl.ds(0, dims), :]) for p in range(block // piece)]
    loads += [
        (solves, held),
        (probes, held2),
        (alpha, line),
        (lengths, scales),
    ]
    loads = [pltpu.make_async_copy(src, dst, load_sem.at[i]) for i, (src, dst) in enumerate(loads)]
    for load in loads:
        load.start()
    for load in loads:
        load.wait()
    extra = line[...].reshape(1, block)
    table = jnp.concatenate([held[...], extra, held2[...], jnp.zeros_like(extra)], 0)
    for p in range(parts):
        msg[p, dims:, :] = table[:, p * piece : (p + 1) * piece]
    pl.semaphore_wait(barrier, len(devices))

    copies = {}
    names = []

    def slot(name):
        if name not in names:
            names.append(name)
        return names.index(name)

    def send(src, name, part, device):
        copy = pltpu.make_async_remote_copy(
            src_ref=src.at[part],
            dst_ref=recv.at[slot(name), part],
            send_sem=send_sem.at[slot(name), part],
            recv_sem=recv_sem.at[slot(name), part],
            device_id=device,
            device_id_type=pl.DeviceIdType.MESH,
        )
        copy.start()
        copies[name, part] = copy

    def arrive(name, part):
        copies[name, part].wait_recv()

    every = range(parts)

    for i, k in enumerate(reaches):
        pl.semaphore_signal(ready.at[i], inc=1, device_id=at(-flip * k), device_id_type=pl.DeviceIdType.MESH)
    for part in every:
        for k in reaches:
            send(msg, ("urgent", k), part, at(-flip * k))
        send(msg, "mate", part, mate)
    for part in every:
        send(msg, "partner", part, partner)

    dim = lax.broadcasted_iota(jnp.int32, (dims, 128), 0)
    length = jnp.full((dims, 128), 1.0, f32)
    for d in range(dims):
        length = jnp.where(dim == d, scales[d], length)
    length = length[:, :1]
    inverse = unit / length

    whole = jnp.concatenate([msg[p] for p in range(parts)], 1)
    field = whole[:dims, :] * inverse
    high, mid, low = pieces(-2.0 * field)
    left_d[...] = jnp.concatenate([high, high, high, norm_rows(field, True), mid, mid, low], 0).T
    row = lax.broadcasted_iota(jnp.int32, (width, block), 0)
    scale = math.e * ln_two / (2.0 * (width - 1))
    top, bottom = whole[dims : dims + width, :], whole[dims + width :, :]
    first = jnp.where(row == width - 1, -math.e * ln_two * top, scale * bottom)
    second = jnp.where(row == width - 1, 0.0, scale * top)
    high, mid, low = pieces(jnp.concatenate([first, second], 0))
    left_c[...] = jnp.concatenate([high, high, high, mid, mid, low], 0).T

    done = []
    pending = []
    contract = (((1,), (1,)), ((), ()))

    def finish(distance, coupling, buffer, lines, fresh):
        distance = jnp.maximum(distance, 1e-30)
        radius = distance * lax.rsqrt(distance)
        power = -inv_ln_two - radius
        weighted = coupling * power * jnp.exp2(power)
        w_high = weighted.astype(bf16)
        w_low = (weighted - w_high.astype(f32)).astype(bf16)
        across = right_d[buffer, : 3 * dims + 16, :]
        part_sum = lax.dot_general(across, w_high, contract, preferred_element_type=f32)
        part_sum += lax.dot_general(across, w_low, contract, preferred_element_type=f32)
        if fresh:
            acc[:, lines] = part_sum
        else:
            acc[:, lines] += part_sum

    def settle():
        while pending:
            which, *rest = pending.pop(0)
            finish(hold_d[which], hold_c[which], *rest)

    def visit(*tiles):
        settle()
        for name, part in tiles:
            buffer, fresh = len(done) % 2, not done
            done.append(0)
            field = recv[slot(name), part, :dims, :] * inverse
            high, mid, low = pieces(field)
            right_d[buffer] = jnp.concatenate([high, mid, low, norm_rows(field, False), high, mid, high], 0)
            table = recv[slot(name), part, dims:, :]
            high, mid, low = pieces(table)
            right_c[buffer] = jnp.concatenate([high, mid, low, high, mid, high], 0)
            for start in range(0, block, chunk):
                lines = pl.ds(start, chunk)
                coupling = jnp.dot(left_c[lines, :], right_c[buffer], preferred_element_type=f32)
                distance = jnp.dot(left_d[lines, :], right_d[buffer], preferred_element_type=f32)
                which = (block - start) // chunk - 1
                if which < kept and (name, part) == tiles[-1]:
                    hold_d[which] = distance
                    hold_c[which] = coupling
                    pending.append((which, buffer, lines, fresh))
                else:
                    finish(distance, coupling, buffer, lines, fresh)

    def land(name, part, onward=None, device=None, source=None):
        arrive(name, part)
        if onward is not None:
            send(recv.at[slot(name) if source is None else source], onward, part, device)

    for part in every:
        land("partner", part)
    visit(*[("partner", part) for part in every])
    for i, k in enumerate(reaches):
        pl.semaphore_wait(ready.at[i], 1)
        for part in every:
            send(msg, ("plain", k), part, at(flip * k))
    last = steps
    inner = [(name, k) for k in reaches if k < last for name in ("urgent", "plain")]
    urgent, plain = ("urgent", last), ("plain", last)
    cross = jnp.where(core == side, slot(urgent), slot(plain))
    for part in every:
        land("mate", part, "mate2", partner)
        land(urgent, part, "over", mate)
        if part:
            land("mate2", part - 1)
            visit(("mate2", part - 1), ("mate", part), (urgent, part))
        else:
            visit(("mate", part), (urgent, part))
    land("mate2", parts - 1)
    visit(("mate2", parts - 1))
    for one in inner:
        for part in every:
            land(one, part, ("over", one), mate)
            send(recv.at[slot(one)], ("core", one), part, partner)
            visit((one, part))
    for part in every:
        land("over", part, "over2", partner)
        land(plain, part, "cross", partner, cross)
        if part:
            land("cross", part - 1)
            land("over2", part - 1)
            visit((plain, part), ("over", part), ("cross", part - 1), ("over2", part - 1))
        else:
            visit((plain, part), ("over", part))
    land("cross", parts - 1)
    land("over2", parts - 1)
    visit(("cross", parts - 1), ("over2", parts - 1))
    for one in inner:
        for part in every:
            land(("over", one), part, ("over2", one), partner)
            land(("core", one), part)
            visit((("over", one), part), (("core", one), part))
            land(("over2", one), part)
            visit((("over2", one), part))
    settle()
    total = acc[...]
    moved = total[:dims] + total[dims : 2 * dims] + total[2 * dims : 3 * dims]
    field = jnp.concatenate([msg[p, :dims, :] for p in range(parts)], 1) * inverse
    out[...] = (-(5.0 / 3.0) / unit / length) * (field * total[3 * dims : 3 * dims + 1] - moved)
    for copy in copies.values():
        copy.wait_send()


def on_device(coords, alpha, probe_solves, probes, lengthscale):
    count = lax.axis_size("blk")
    steps = count // 4
    dims, block = coords.shape
    table_rows = 2 * (probes.shape[0] + 1)
    rows = dims + table_rows
    depth_d, depth_c = 6 * dims + 16, 6 * table_rows
    parts = block // piece
    return pl.pallas_call(
        functools.partial(kernel, dims, steps, count),
        out_shape=pltpu.VMEM((dims, block), f32),
        in_specs=[pl.BlockSpec(memory_space=pltpu.HBM)] * 5,
        out_specs=pl.BlockSpec(memory_space=pltpu.VMEM),
        scratch_shapes=[
            pltpu.VMEM((parts, rows, piece), f32),
            pltpu.VMEM((block,), f32),
            pltpu.VMEM(probes.shape, f32),
            pltpu.VMEM(probes.shape, f32),
            pltpu.SMEM((dims,), f32),
            pltpu.VMEM((2 * steps, parts, rows, piece), f32),
            pltpu.VMEM((block, depth_d), bf16),
            pltpu.VMEM((block, depth_c), bf16),
            pltpu.VMEM((2, depth_d, piece), bf16),
            pltpu.VMEM((2, depth_c, piece), bf16),
            pltpu.VMEM((kept, chunk, piece), f32),
            pltpu.VMEM((kept, chunk, piece), f32),
            pltpu.VMEM((3 * dims + 16, block), f32),
            pltpu.SemaphoreType.DMA((parts + 4,)),
            pltpu.SemaphoreType.REGULAR((steps // 4,)),
            pltpu.SemaphoreType.DMA((2 * steps, parts)),
            pltpu.SemaphoreType.DMA((2 * steps, parts)),
        ],
        compiler_params=pltpu.CompilerParams(collective_id=0, has_side_effects=True),
    )(coords, alpha, probe_solves, probes, lengthscale)


def solution(mesh):
    return jax.shard_map(
        on_device,
        mesh=mesh,
        in_specs=(
            P(None, ("groups", "blk")),
            P(("groups", "blk")),
            P(None, ("groups", "blk")),
            P(None, ("groups", "blk")),
            P(),
        ),
        out_specs=P(None, ("groups", "blk")),
        check_vma=False,
    )
```
